128 devices in a mesh: slab: 8 (over z, core), tile: 16 (over x, y).
Axes of the slice: x: 4, y: 4, z: 4, core: 2. Of those that a mesh axis runs over, the one named last changes fastest.
Arguments:
- coarse: bfloat16 [192, 32, 64, 64], P(None, 'slab', 'tile'), may hold values from -6 to 6
- up_weight: bfloat16 [3, 3, 96, 192], replicated, may hold values from -0.15625 to 0.15625
- up_bias: float32 [96], replicated, may hold values from -3 to 3
- gain_one: float32 [96], replicated, may hold values from 0.1 to 1.9
- conv_one: bfloat16 [3, 3, 96, 288], replicated, may hold values from -0.125 to 0.125
- bias_one: float32 [96], replicated, may hold values from -3 to 3
- gain_two: float32 [96], replicated, may hold values from 0.1 to 1.9
- conv_two: bfloat16 [3, 3, 96, 288], replicated, may hold values from -0.125 to 0.125
- bias_two: float32 [96], replicated, may hold values from -3 to 3
Outputs:
- decoded: bfloat16 [96, 32, 128, 128], P(None, 'slab', 'tile')
The draws below stay inside these ranges and needn't reach their ends.
All inputs are finite; a program needn't handle non-finite values.
Results may differ from the reference program's by a relative error of at most 0.009.
Values may be sent and summed in bfloat16 or wider, within the bound.
No kernel may reach another device: no remote copies, remote signals or barrier semaphores. Data moves between devices by JAX's collectives and lax.ppermute only.
A program may use at most 64 MiB of HBM per device.

```python
import jax
import jax.numpy as jnp
from jax import lax

COARSE_CH = 192
FINE_CH = 96
COLS = 128
FRAMES = 32
ROWS = 128


def steps_of(key, dims, shards, low, largest):
    def one(dim, shards_of):
        heights = jax.random.uniform(jax.random.fold_in(jax.random.fold_in(key, 6), dim), (shards_of,), jnp.float32, low / len(shards), largest / len(shards))
        return jnp.repeat(jnp.exp(heights), dims[dim] // shards_of).reshape((-1,) + (1,) * (len(dims) - dim - 1))

    loudness = one(*shards[0])
    for cut in shards[1:]:
        loudness = loudness * one(*cut)
    return loudness


def bell_draw(stream_key, shape, width, limit, pieces=(), dtype=jnp.bfloat16):
    values = width * jax.random.normal(stream_key, shape, jnp.float32)
    if pieces:
        values = values * steps_of(stream_key, shape, pieces, -0.22, 0.18)
    return jnp.clip(values, -limit, limit).astype(dtype)


def setup_inputs(seed: int = 0) -> dict:
    arg_keys = jax.random.split(jax.random.key(seed), 10)
    coarse = bell_draw(arg_keys[0], (COARSE_CH, FRAMES, ROWS // 2, COLS // 2), 1.0, 6.0, ((1, 8), (2, 16)))
    up_weight = bell_draw(arg_keys[1], (3, 3, FINE_CH, COARSE_CH), (9 * COARSE_CH) ** -0.5, 0.15625)
    up_bias = bell_draw(arg_keys[2], (FINE_CH,), 0.5, 3.0, (), jnp.float32)
    gain_one = jnp.clip(1.0 + 0.18 * jax.random.normal(arg_keys[3], (FINE_CH,), jnp.float32), 0.1, 1.9)
    conv_one = bell_draw(arg_keys[4], (3, 3, FINE_CH, 3 * FINE_CH), (27 * FINE_CH) ** -0.5, 0.125)
    bias_one = bell_draw(arg_keys[5], (FINE_CH,), 0.5, 3.0, (), jnp.float32)
    gain_two = jnp.clip(1.0 + 0.18 * jax.random.normal(arg_keys[6], (FINE_CH,), jnp.float32), 0.1, 1.9)
    conv_two = bell_draw(arg_keys[7], (3, 3, FINE_CH, 3 * FINE_CH), (27 * FINE_CH) ** -0.5, 0.125)
    bias_two = bell_draw(arg_keys[8], (FINE_CH,), 0.5, 3.0, (), jnp.float32)
    return {"coarse": coarse, "up_weight": up_weight, "up_bias": up_bias, "gain_one": gain_one, "conv_one": conv_one, "bias_one": bias_one, "gain_two": gain_two, "conv_two": conv_two, "bias_two": bias_two}


def norm_act(values, gain):
    meansq = lax.optimization_barrier(jnp.mean(values * values, axis=0, keepdims=True))
    scaled = values * lax.rsqrt(meansq + 1e-06) * gain[:, None, None, None]
    return (scaled * jax.nn.sigmoid(scaled)).astype(jnp.bfloat16)

def conv_frame(window, weight, bias):
    chans = window.shape[0]
    padded = jnp.pad(window, ((0, 0), (0, 0), (1, 1), (1, 1)))
    height = padded.shape[2] - 2
    breadth = padded.shape[3] - 2
    summed = jnp.zeros((weight.shape[2], height * breadth), jnp.float32)
    for t_tap in range(3):
        for h_tap in range(3):
            stacked = jnp.concatenate([padded[:, t_tap, h_tap:h_tap + height, w_tap:w_tap + breadth] for w_tap in range(3)], axis=0)
            summed = summed + jnp.dot(weight[t_tap, h_tap], stacked.reshape(3 * chans, -1), preferred_element_type=jnp.float32)
    return summed.reshape(-1, 1, height, breadth) + bias[:, None, None, None]

def plane_frame(padded, weight, bias):
    chans = padded.shape[0]
    height = padded.shape[1] - 2
    breadth = padded.shape[2] - 2
    summed = jnp.zeros((weight.shape[2], height * breadth), jnp.float32)
    for h_tap in range(3):
        for w_tap in range(3):
            window = padded[:, h_tap:h_tap + height, w_tap:w_tap + breadth].reshape(chans, -1)
            summed = summed + jnp.dot(weight[h_tap, w_tap], window, preferred_element_type=jnp.float32)
    return summed.reshape(-1, 1, height, breadth) + bias[:, None, None, None]

def reference(coarse, up_weight, up_bias, gain_one, conv_one, bias_one, gain_two, conv_two, bias_two):
    chans = up_weight.shape[2]
    height = coarse.shape[2] * 2
    breadth = coarse.shape[3] * 2
    frames_first = jnp.moveaxis(coarse, 1, 0)

    def advance(carry, frame):
        past_one, past_two = carry
        enlarged = jnp.repeat(jnp.repeat(frame, 2, axis=1), 2, axis=2)
        enlarged = jnp.pad(enlarged, ((0, 0), (1, 1), (1, 1)))
        upsampled = plane_frame(enlarged, up_weight, up_bias).astype(jnp.bfloat16)
        first_act = norm_act(upsampled.astype(jnp.float32), gain_one)
        window_one = jnp.concatenate([past_one, first_act], axis=1)
        hidden = conv_frame(window_one, conv_one, bias_one)
        second_act = norm_act(hidden, gain_two)
        window_two = jnp.concatenate([past_two, second_act], axis=1)
        result = upsampled.astype(jnp.float32) + conv_frame(window_two, conv_two, bias_two)
        return ((window_one[:, 1:], window_two[:, 1:]), result[:, 0].astype(jnp.bfloat16))
    start = (jnp.zeros((chans, 2, height, breadth), jnp.bfloat16), jnp.zeros((chans, 2, height, breadth), jnp.bfloat16))
    final, outputs = lax.scan(advance, start, frames_first)
    return jnp.moveaxis(outputs, 0, 1)
```

```python
import jax
import jax.numpy as jnp
import numpy as np
from jax import lax
from jax.experimental import pallas as pl
from jax.experimental.pallas import tpu as pltpu
from jax.sharding import PartitionSpec as P

F32 = jnp.float32
BF16 = jnp.bfloat16
CH = 96


def silu(y):
    return y * (0.5 + 0.5 * jnp.tanh(0.5 * y))


def norm_act(v, gain):
    meansq = jnp.sum(v * v, axis=0, keepdims=True) * (1.0 / CH)
    return silu(v * lax.rsqrt(meansq + 1e-06) * gain)


def lanes_of(shape):
    return lax.broadcasted_iota(jnp.int32, shape, 1)


def spread_matrix():
    m = np.zeros((256, 256), np.float32)
    for q in range(2):
        for f in range(2):
            for j in range(64):
                m[q * 128 + f * 64 + j, f * 128 + 2 * j + q] = 1
    return m


def up_stage(x_ref, wup_ref, spread_ref, bias_ref, gain_ref, act_ref, first, raw_ref, valid):
    low = lanes_of((CH, 128)) % 64 == 0
    high = lanes_of((CH, 128)) % 64 == 63

    def row(i, carry):
        for p in range(2):
            top = x_ref[:, i + p].reshape(256, 192)
            bottom = x_ref[:, i + p + 1].reshape(256, 192)
            dims = (((1,), (1,)), ((), ()))
            u = lax.dot_general(wup_ref[2 * p], top, dims, preferred_element_type=F32)
            u = u + lax.dot_general(wup_ref[2 * p + 1], bottom, dims, preferred_element_type=F32)
            stacked = []
            for g in range(2):
                part = u[:, 128 * g:128 * g + 128]
                even = part[:CH] + jnp.where(low, 0.0, pltpu.roll(part[CH:2 * CH], 1, 1)) + bias_ref[...]
                odd = part[2 * CH:3 * CH] + jnp.where(high, 0.0, pltpu.roll(part[3 * CH:], 127, 1)) + bias_ref[...]
                stacked.append(jnp.concatenate([even.astype(BF16), odd.astype(BF16)], axis=1))
            fine = jnp.dot(jnp.concatenate(stacked, axis=0), spread_ref[...], preferred_element_type=F32)
            for g in range(2):
                for h in range(2):
                    v = fine[CH * g:CH * g + CH, 128 * h:128 * h + 128]
                    if raw_ref is not None:
                        raw_ref[2 * g + h, 2 * i + p] = v.astype(BF16)
                    act = jnp.where(valid(i), norm_act(v, gain_ref[...]), 0.0)
                    act_ref[first + 2 * g + h, 2 * i + p] = act.astype(BF16)
        return carry

    lax.fori_loop(0, 6, row, 0)


def conv_pair(src_ref, w_ref, f, r):
    taps = [
        jnp.concatenate([src_ref[f + t, r + a], src_ref[f + t, r + a + 1]], axis=1)
        for t in range(3) for a in range(3)
    ]
    s = jnp.dot(w_ref[...], jnp.concatenate(taps, axis=0), preferred_element_type=F32)
    lane = lanes_of((CH, 128))
    rows = []
    for h in range(2):
        part = s[:, 128 * h:128 * h + 128]
        left = jnp.where(lane == 0, 0.0, pltpu.roll(part[:CH], 1, 1))
        right = jnp.where(lane == 127, 0.0, pltpu.roll(part[2 * CH:], 127, 1))
        rows.append(left + part[CH:2 * CH] + right)
    return rows


def conv_one_stage(act_ref, w_ref, bias_ref, gain_ref, hid_ref, low, high, valid):
    def frame(f, carry):
        for pair in range(5):
            rows = conv_pair(act_ref, w_ref, f, 2 * pair)
            for h in range(2):
                q = 2 * pair + h
                act = norm_act(rows[h] + bias_ref[...], gain_ref[...])
                act = jnp.where(valid(f, q), act, 0.0)
                hid_ref[f, q] = act.astype(BF16)
        return carry

    lax.fori_loop(low, high, frame, 0)


def conv_two_stage(hid_ref, w_ref, bias_ref, raw_ref, out_ref, mix_ref):
    def frame(f, carry):
        for pair in range(4):
            rows = conv_pair(hid_ref, w_ref, f, 2 * pair)
            for h in range(2):
                r = 2 * pair + h
                res = raw_ref[f, r + 2].astype(F32) + rows[h] + bias_ref[...]
                mix_ref[pl.ds(r, CH, stride=8), :] = res
        out_ref[:, f] = mix_ref[...].reshape(CH, 8, 128).astype(BF16)
        return carry

    lax.fori_loop(0, 4, frame, 0)


def whole_kernel(flags, own_ref, old_ref, wup_ref, spread_ref, upb_ref, g1_ref, w1_ref, b1_ref, g2_ref, w2_ref, b2_ref,
                 out_ref, act_ref, hid_ref, raw_ref, mix_ref):
    has_top, has_bottom, has_old = flags[0] > 0, flags[1] > 0, flags[2] > 0

    def in_image(i, last):
        return jnp.logical_and(jnp.logical_or(i > 0, has_top), jnp.logical_or(i < last, has_bottom))

    up_stage(own_ref, wup_ref, spread_ref, upb_ref, g1_ref, act_ref, 4, raw_ref, lambda i: in_image(i, 5))
    up_stage(old_ref, wup_ref, spread_ref, upb_ref, g1_ref, act_ref, 0, None,
             lambda i: jnp.logical_and(in_image(i, 5), has_old))

    def hidden_valid(f, q):
        ok = jnp.logical_or(f >= 2, has_old)
        if q == 0:
            ok = jnp.logical_and(ok, has_top)
        if q == 9:
            ok = jnp.logical_and(ok, has_bottom)
        return ok

    conv_one_stage(act_ref, w1_ref, b1_ref, g2_ref, hid_ref, 0, 6, hidden_valid)
    conv_two_stage(hid_ref, w2_ref, b2_ref, raw_ref, out_ref, mix_ref)


def up_weights(w):
    w = w.astype(F32)
    rows = [w[0], w[1] + w[2], w[0] + w[1], w[2]]
    return jnp.stack([
        jnp.concatenate([r[1] + r[2], r[0], r[0] + r[1], r[2]], axis=0) for r in rows
    ]).astype(BF16)


def conv_weights(w):
    return w.reshape(3, 3, CH, 3, CH).transpose(3, 2, 0, 1, 4).reshape(3 * CH, 9 * CH)


def column(v):
    return jnp.broadcast_to(v[:, None], (CH, 128))


def shards(coarse, up_weight, up_bias, gain_one, conv_one, bias_one, gain_two, conv_two, bias_two):
    tiles, slabs = lax.axis_size("tile"), lax.axis_size("slab")
    x = coarse.transpose(1, 2, 3, 0)
    above = lax.ppermute(x[:, 2:], "tile", [(i, i + 1) for i in range(tiles - 1)])
    below = lax.ppermute(x[:, :2], "tile", [(i + 1, i) for i in range(tiles - 1)])
    own = jnp.concatenate([above, x, below], axis=1)
    old = lax.ppermute(own, "slab", [(i, i + 1) for i in range(slabs - 1)])
    place, age = lax.axis_index("tile"), lax.axis_index("slab")
    flags = jnp.stack([place, tiles - 1 - place, age]).astype(jnp.int32)
    vmem = pl.BlockSpec(memory_space=pltpu.VMEM)
    return pl.pallas_call(
        whole_kernel,
        out_shape=jax.ShapeDtypeStruct((CH, 4, 8, 128), BF16),
        in_specs=[pl.BlockSpec(memory_space=pltpu.SMEM)] + [vmem] * 11,
        out_specs=vmem,
        scratch_shapes=[
            pltpu.VMEM((8, 12, CH, 128), BF16),
            pltpu.VMEM((6, 10, CH, 128), BF16),
            pltpu.VMEM((4, 12, CH, 128), BF16),
            pltpu.VMEM((CH * 8, 128), F32),
        ],
        compiler_params=pltpu.CompilerParams(vmem_limit_bytes=48 << 20),
        name="decode",
    )(flags, own, old, up_weights(up_weight), jnp.asarray(spread_matrix(), BF16), column(up_bias), column(gain_one),
      conv_weights(conv_one), column(bias_one), column(gain_two), conv_weights(conv_two), column(bias_two))


def solution(mesh):
    return jax.shard_map(
        shards,
        mesh=mesh,
        in_specs=(P(None, "slab", "tile", None), P(), P(), P(), P(), P(), P(), P(), P()),
        out_specs=P(None, "slab", "tile", None),
        check_vma=False,
    )
```

```python
import jax
import jax.numpy as jnp
import numpy as np
from jax import lax
from jax.experimental import pallas as pl
from jax.experimental.pallas import tpu as pltpu
from jax.sharding import PartitionSpec as P

F32 = jnp.float32
BF16 = jnp.bfloat16
CH = 96
VMEM = pl.BlockSpec(memory_space=pltpu.VMEM)
SMEM = pl.BlockSpec(memory_space=pltpu.SMEM)
ANY = pl.BlockSpec(memory_space=pl.ANY)


def silu(y):
    return y * (0.5 + 0.5 * jnp.tanh(0.5 * y))


def norm_act(v, gain):
    meansq = jnp.sum(v * v, axis=0, keepdims=True) * (1.0 / CH)
    return silu(v * lax.rsqrt(meansq + 1e-06) * gain)


def lanes_of(shape):
    return lax.broadcasted_iota(jnp.int32, shape, 1)


def spread_matrix():
    m = np.zeros((256, 256), np.float32)
    for q in range(2):
        for f in range(2):
            for j in range(64):
                m[q * 128 + f * 64 + j, f * 128 + 2 * j + q] = 1
    return m


def prep_kernel(up_ref, one_ref, two_ref, upb_ref, g1_ref, b1_ref, g2_ref, b2_ref, wup_ref, w1_ref, w2_ref, cols_ref):
    for n in range(4):
        taps = []
        for b in range(3):
            if n == 0:
                tap = up_ref[0, b].astype(F32)
            elif n == 3:
                tap = up_ref[2, b].astype(F32)
            else:
                tap = up_ref[1, b].astype(F32) + up_ref[2 if n == 1 else 0, b].astype(F32)
            taps.append(tap)
        for m, tap in enumerate((taps[1] + taps[2], taps[0], taps[0] + taps[1], taps[2])):
            wup_ref[n, CH * m:CH * m + CH, :] = tap.astype(BF16)
    for src_ref, dst_ref in ((one_ref, w1_ref), (two_ref, w2_ref)):
        for b in range(3):
            pieces = [src_ref[t, a][:, CH * b:CH * b + CH] for t in range(3) for a in range(3)]
            dst_ref[CH * b:CH * b + CH, :] = jnp.concatenate(pieces, axis=1)
    for n, ref in enumerate((upb_ref, g1_ref, b1_ref, g2_ref, b2_ref)):
        cols_ref[n] = jnp.broadcast_to(ref[...], (128, CH)).T


def up_tile(blocks, p, x_ref, wup_ref, spread_ref, bias, gain, emit):
    low = lanes_of((CH, 128)) % 64 == 0
    high = lanes_of((CH, 128)) % 64 == 63
    dims = (((1,), (1,)), ((), ()))
    u = lax.dot_general(wup_ref[2 * p], blocks(p), dims, preferred_element_type=F32)
    u = u + lax.dot_general(wup_ref[2 * p + 1], blocks(p + 1), dims, preferred_element_type=F32)
    stacked = []
    for g in range(2):
        part = u[:, 128 * g:128 * g + 128]
        even = part[:CH] + jnp.where(low, 0.0, pltpu.roll(part[CH:2 * CH], 1, 1)) + bias
        odd = part[2 * CH:3 * CH] + jnp.where(high, 0.0, pltpu.roll(part[3 * CH:], 127, 1)) + bias
        stacked.append(jnp.concatenate([even.astype(BF16), odd.astype(BF16)], axis=1))
    fine = jnp.dot(jnp.concatenate(stacked, axis=0), spread_ref[...], preferred_element_type=F32)
    for g in range(2):
        for h in range(2):
            emit(g, h, fine[CH * g:CH * g + CH, 128 * h:128 * h + 128])


def conv_pair(src, w_ref, f, r):
    taps = [
        jnp.concatenate([src(f + t, r + a), src(f + t, r + a + 1)], axis=1)
        for t in range(3) for a in range(3)
    ]
    s = jnp.dot(w_ref[...], jnp.concatenate(taps, axis=0), preferred_element_type=F32)
    lane = lanes_of((CH, 128))
    rows = []
    for h in range(2):
        part = s[:, 128 * h:128 * h + 128]
        left = jnp.where(lane == 0, 0.0, pltpu.roll(part[:CH], 1, 1))
        right = jnp.where(lane == 127, 0.0, pltpu.roll(part[2 * CH:], 127, 1))
        rows.append(left + part[CH:2 * CH] + right)
    return rows


def hidden_frame(act_ref, f, w_ref, bias, gain, hid_ref, to, has_top, has_bottom):
    for pair in range(5):
        rows = conv_pair(lambda i, r: act_ref[i, r], w_ref, f, 2 * pair)
        for h in range(2):
            q = 2 * pair + h
            act = norm_act(rows[h] + bias, gain)
            if q == 0:
                act = jnp.where(has_top, act, 0.0)
            if q == 9:
                act = jnp.where(has_bottom, act, 0.0)
            hid_ref[to, q] = act.astype(BF16)


def decoded_frame(hid_ref, f, w_ref, bias, raw_ref, n, mix_ref, res_ref, to):
    for pair in range(4):
        rows = conv_pair(lambda i, r: hid_ref[i, r], w_ref, f, 2 * pair)
        for h in range(2):
            r = 2 * pair + h
            mix_ref[pl.ds(r, CH, stride=8), :] = raw_ref[n, r].astype(F32) + rows[h] + bias
    res_ref[:, to] = mix_ref[...].reshape(CH, 8, 128).astype(BF16)


def in_image(i, has_top, has_bottom):
    return jnp.logical_and(jnp.logical_or(i > 0, has_top), jnp.logical_or(i < 5, has_bottom))


def first_kernel(flags, x_ref, above_ref, below_ref, wup_ref, spread_ref, w1_ref, cols_ref,
                 act_ref, raw_ref, hid_ref, own_ref):
    has_top, has_bottom = flags[0] > 0, flags[1] > 0
    own_ref[:, :2] = above_ref[...]
    own_ref[:, 2:6] = x_ref[...]
    own_ref[:, 6:] = below_ref[...]

    def row(i, carry):
        ok = in_image(i, has_top, has_bottom)
        for p in range(2):
            def emit(g, h, v, p=p):
                raw_ref[2 * g + h, 2 * i + p] = v.astype(BF16)
                act_ref[2 * g + h, 2 * i + p] = jnp.where(ok, norm_act(v, cols_ref[1]), 0.0).astype(BF16)

            up_tile(lambda d: own_ref[:, i + d].reshape(256, 192), p, None, wup_ref, spread_ref, cols_ref[0], None, emit)
        return carry

    lax.fori_loop(0, 6, row, 0)

    def frame(f, carry):
        hidden_frame(act_ref, f, w1_ref, cols_ref[2], cols_ref[3], hid_ref, f, has_top, has_bottom)
        return carry

    lax.fori_loop(0, 2, frame, 0)


def second_kernel(flags, old_ref, wup_ref, spread_ref, w1_ref, w2_ref, cols_ref, act_ref, raw_ref, new_ref,
                  hid_ref, out_ref, all_act_ref, all_hid_ref, mix_ref, res_ref, sem):
    has_top, has_bottom, has_old = flags[0] > 0, flags[1] > 0, flags[2] > 0
    all_act_ref[2:] = act_ref[:2]
    all_hid_ref[2:] = new_ref[...]

    def row(k, carry):
        i = 2 * k
        for p in range(2):
            def emit(g, h, v, p=p):
                ok = jnp.logical_and(in_image(i + h, has_top, has_bottom), has_old)
                all_act_ref[g, 2 * (i + h) + p] = jnp.where(ok, norm_act(v, cols_ref[1]), 0.0).astype(BF16)

            up_tile(lambda d: old_ref[:, pl.ds(i + d, 2)].reshape(256, 192), p, None, wup_ref, spread_ref, cols_ref[0],
                    None, emit)
        return carry

    lax.fori_loop(0, 3, row, 0)

    def frame(f, carry):
        hidden_frame(all_act_ref, f, w1_ref, cols_ref[2], cols_ref[3], all_hid_ref, f, has_top, has_bottom)
        return carry

    lax.fori_loop(0, 2, frame, 0)
    hid_ref[...] = all_hid_ref[:2]

    def result(f, carry):
        decoded_frame(all_hid_ref, f, w2_ref, cols_ref[4], raw_ref, f, mix_ref, res_ref, f)
        return carry

    lax.fori_loop(0, 2, result, 0)
    copy = pltpu.make_async_copy(res_ref, out_ref.at[:, 2:4], sem)
    copy.start()
    copy.wait()


def third_kernel(flags, w2_ref, cols_ref, raw_ref, past_ref, hid_ref, _, out_ref, all_hid_ref, mix_ref, res_ref, sem):
    all_hid_ref[:2] = jnp.where(flags[2] > 0, past_ref[...], 0)
    all_hid_ref[2:] = hid_ref[...]

    def result(f, carry):
        decoded_frame(all_hid_ref, f, w2_ref, cols_ref[4], raw_ref, f, mix_ref, res_ref, f)
        return carry

    lax.fori_loop(0, 2, result, 0)
    copy = pltpu.make_async_copy(res_ref, out_ref.at[:, :2], sem)
    copy.start()
    copy.wait()


def shape(*dims, dtype=BF16):
    return jax.ShapeDtypeStruct(dims, dtype)


def call(kernel, name, flops, in_specs, out_shape, out_specs, scratch=(), **kw):
    return pl.pallas_call(
        kernel,
        out_shape=out_shape,
        in_specs=in_specs,
        out_specs=out_specs,
        scratch_shapes=list(scratch),
        compiler_params=pltpu.CompilerParams(vmem_limit_bytes=48 << 20),
        cost_estimate=pl.CostEstimate(flops=flops, transcendentals=0, bytes_accessed=4 << 20),
        name=name,
        **kw,
    )


def shards(coarse, up_weight, up_bias, gain_one, conv_one, bias_one, gain_two, conv_two, bias_two):
    tiles, slabs = lax.axis_size("tile"), lax.axis_size("slab")
    later = [(i, i + 1) for i in range(slabs - 1)]
    x = coarse.transpose(1, 2, 3, 0)
    above = lax.ppermute(x[:, 2:], "tile", [(i, i + 1) for i in range(tiles - 1)])
    below = lax.ppermute(x[:, :2], "tile", [(i + 1, i) for i in range(tiles - 1)])
    wup, w1, w2, cols = call(
        prep_kernel, "prep", 1 << 30, [VMEM] * 8,
        (shape(4, 4 * CH, 192), shape(3 * CH, 9 * CH), shape(3 * CH, 9 * CH), shape(5, CH, 128, dtype=F32)), (VMEM,) * 4,
    )(up_weight, conv_one, conv_two, *(v.reshape(1, CH) for v in (up_bias, gain_one, bias_one, gain_two, bias_two)))
    spread = jnp.asarray(spread_matrix(), BF16)
    place, age = lax.axis_index("tile"), lax.axis_index("slab")
    flags = jnp.stack([place, tiles - 1 - place, age]).astype(jnp.int32)
    old = lax.ppermute(jnp.concatenate([above[2:], x[2:], below[2:]], axis=1), "slab", later)
    act, raw, new = call(
        first_kernel, "first", 3 << 30, [SMEM] + [VMEM] * 7,
        (shape(4, 12, CH, 128), shape(4, 12, CH, 128), shape(2, 10, CH, 128)), (VMEM,) * 3,
        [pltpu.VMEM((4, 8, 64, 192), BF16)],
    )(flags, x, above, below, wup, spread, w1, cols)
    past = lax.ppermute(new, "slab", later)
    hid, out = call(
        second_kernel, "second", 3 << 30, [SMEM] + [VMEM] * 9,
        (shape(2, 10, CH, 128), shape(CH, 4, 8, 128)), (VMEM, ANY),
        [pltpu.VMEM((4, 12, CH, 128), BF16), pltpu.VMEM((4, 10, CH, 128), BF16), pltpu.VMEM((CH * 8, 128), F32),
         pltpu.VMEM((CH, 2, 8, 128), BF16), pltpu.SemaphoreType.DMA],
    )(flags, old, wup, spread, w1, w2, cols, act, raw[2:, 2:10], new)
    return call(
        third_kernel, "third", 1 << 30, [SMEM] + [VMEM] * 5 + [ANY],
        shape(CH, 4, 8, 128), ANY,
        [pltpu.VMEM((4, 10, CH, 128), BF16), pltpu.VMEM((CH * 8, 128), F32),
         pltpu.VMEM((CH, 2, 8, 128), BF16), pltpu.SemaphoreType.DMA],
        input_output_aliases={6: 0},
    )(flags, w2, cols, raw[:2, 2:10], past, hid, out)


def solution(mesh):
    return jax.shard_map(
        shards,
        mesh=mesh,
        in_specs=(P(None, "slab", "tile", None), P(), P(), P(), P(), P(), P(), P(), P()),
        out_specs=P(None, "slab", "tile", None),
        check_vma=False,
    )
```

```python
import jax
import jax.numpy as jnp
import numpy as np
from jax import lax
from jax.experimental import pallas as pl
from jax.experimental.pallas import tpu as pltpu
from jax.sharding import PartitionSpec as P

F32 = jnp.float32
BF16 = jnp.bfloat16
CH = 96
VMEM = pl.BlockSpec(memory_space=pltpu.VMEM)
SMEM = pl.BlockSpec(memory_space=pltpu.SMEM)
ANY = pl.BlockSpec(memory_space=pl.ANY)
HBM = pl.BlockSpec(memory_space=pltpu.HBM)


def silu(y):
    return y * (0.5 + 0.5 * jnp.tanh(0.5 * y))


def norm_act(v, gain):
    meansq = jnp.sum(v * v, axis=0, keepdims=True) * (1.0 / CH)
    return silu(v * lax.rsqrt(meansq + 1e-06) * gain)


def lanes_of(shape):
    return lax.broadcasted_iota(jnp.int32, shape, 1)


def weave_matrix():
    m = np.zeros((256, 256), np.float32)
    for h in range(2):
        for q in range(2):
            for j in range(64):
                m[h * 128 + q * 64 + j, h * 128 + 2 * j + q] = 1
    return m


def up_tile(top, bottom, p, wup_ref, cols_ref, emit):
    lane = lanes_of((CH, 128))
    dims = (((1,), (1,)), ((), ()))
    u = lax.dot_general(wup_ref[2 * p], top.reshape(256, 192), dims, preferred_element_type=F32)
    u = u + lax.dot_general(wup_ref[2 * p + 1], bottom.reshape(256, 192), dims, preferred_element_type=F32)
    for g in range(2):
        part = u[:, 128 * g:128 * g + 128]
        even = part[:CH] + jnp.where(lane % 64 == 0, 0.0, pltpu.roll(part[CH:2 * CH], 1, 1)) + cols_ref[0]
        odd = part[2 * CH:3 * CH] + jnp.where(lane % 64 == 63, 0.0, pltpu.roll(part[3 * CH:], 127, 1)) + cols_ref[0]
        even, odd = even.astype(BF16).astype(F32), odd.astype(BF16).astype(F32)
        emit(2 * g, jnp.where(lane < 64, even, pltpu.roll(odd, 64, 1)))
        emit(2 * g + 1, jnp.where(lane < 64, pltpu.roll(even, 64, 1), odd))


def conv_pair(src, w_ref, f, r):
    taps = [
        jnp.concatenate([src(f + t, r + a), src(f + t, r + a + 1)], axis=1)
        for t in range(3) for a in range(3)
    ]
    s = jnp.dot(w_ref[...], jnp.concatenate(taps, axis=0), preferred_element_type=F32)
    lane = lanes_of((CH, 128))
    edge = jnp.logical_or(lane == 0, lane == 127)
    rows = []
    for h in range(2):
        part = s[:, 128 * h:128 * h + 128]
        left, right = part[:CH], part[2 * CH:]
        near = pltpu.roll(jnp.where(lane < 64, left, right), 64, 1)
        far = jnp.where(lane < 64, right, left)
        far = jnp.where(lane < 64, pltpu.roll(far, 65, 1), pltpu.roll(far, 63, 1))
        rows.append(part[CH:2 * CH] + near + jnp.where(edge, 0.0, far))
    return rows


def hidden_frame(src, f, w_ref, cols_ref, hid_ref, has_top, has_bottom):
    for pair in range(5):
        rows = conv_pair(src, w_ref, f, 2 * pair)
        for h in range(2):
            q = 2 * pair + h
            act = norm_act(rows[h] + cols_ref[2], cols_ref[3])
            if q == 0:
                act = jnp.where(has_top, act, 0.0)
            if q == 9:
                act = jnp.where(has_bottom, act, 0.0)
            hid_ref[f, q] = act.astype(BF16)


def decoded_frames(src, w_ref, weave_ref, cols_ref, raw, both_ref, mix_ref, res_ref, out_ref, start, sems):
    copies = []

    def finish(f):
        woven = jnp.dot(both_ref[f], weave_ref[...], preferred_element_type=F32)
        for r in range(8):
            at, h = CH * (r // 2), 128 * (r % 2)
            mix_ref[f, pl.ds(r, CH, stride=8), :] = woven[at:at + CH, h:h + 128]
        res_ref[:, f] = mix_ref[f].reshape(CH, 8, 128).astype(BF16)
        copies.append(pltpu.make_async_copy(res_ref.at[:, f], out_ref.at[:, start + f], sems.at[f]))
        copies[f].start()

    for n in range(8):
        f, pair = n // 4, n % 4
        rows = conv_pair(src, w_ref, f, 2 * pair)
        res = [raw(f, 2 * pair + h).astype(F32) + rows[h] + cols_ref[4] for h in range(2)]
        both_ref[f, CH * pair:CH * pair + CH] = jnp.concatenate([v.astype(BF16) for v in res], axis=1)
        if n == 5:
            finish(0)
    finish(1)
    for copy in copies:
        copy.wait()


def prep_kernel(x_ref, up_ref, one_ref, two_ref, upb_ref, g1_ref, b1_ref, g2_ref, b2_ref,
                wup_ref, w1_ref, w2_ref, cols_ref, act_ref, raw_ref, one_buf, two_buf, sems):
    loads = [
        pltpu.make_async_copy(one_ref, one_buf, sems.at[0]),
        pltpu.make_async_copy(two_ref, two_buf, sems.at[1]),
    ]
    for load in loads:
        load.start()
    for n in range(4):
        taps = []
        for b in range(3):
            if n == 0:
                tap = up_ref[0, b].astype(F32)
            elif n == 3:
                tap = up_ref[2, b].astype(F32)
            else:
                tap = up_ref[1, b].astype(F32) + up_ref[2 if n == 1 else 0, b].astype(F32)
            taps.append(tap)
        for m, tap in enumerate((taps[1] + taps[2], taps[0], taps[0] + taps[1], taps[2])):
            wup_ref[n, CH * m:CH * m + CH, :] = tap.astype(BF16)
    for n, ref in enumerate((upb_ref, g1_ref, b1_ref, g2_ref, b2_ref)):
        cols_ref[n] = jnp.broadcast_to(ref[...], (128, CH)).T
    for k in range(3):
        for n, p in enumerate((1, 0)):
            def emit(f, v, to=2 * k + n):
                raw_ref[f, to] = v.astype(BF16)
                act_ref[f, to] = norm_act(v, cols_ref[1]).astype(BF16)

            up_tile(x_ref[:, k], x_ref[:, k + 1], p, wup_ref, cols_ref, emit)
    for load, src_ref, dst_ref in ((loads[0], one_buf, w1_ref), (loads[1], two_buf, w2_ref)):
        load.wait()
        for b in range(3):
            pieces = [src_ref[t, a][:, CH * b:CH * b + CH] for t in range(3) for a in range(3)]
            dst_ref[CH * b:CH * b + CH, :] = jnp.concatenate(pieces, axis=1)


def first_kernel(flags, x_ref, above_ref, below_ref, wup_ref, w1_ref, cols_ref, inner_ref,
                 act_ref, edge_ref, hid_ref):
    has_top, has_bottom = flags[0] > 0, flags[1] > 0
    act_ref[:, 3:9] = inner_ref[...]
    above, below = above_ref[...], below_ref[...]
    above, below = (above[..., :192], above[..., 192:]), (below[..., :192], below[..., 192:])
    tiles = (
        (0, above[0], above[1], 0, has_top, None),
        (1, above[1], x_ref[:, 0], 1, has_top, None),
        (2, above[1], x_ref[:, 0], 0, None, 0),
        (9, x_ref[:, 3], below[0], 1, None, 1),
        (10, x_ref[:, 3], below[0], 0, has_bottom, None),
        (11, below[0], below[1], 1, has_bottom, None),
    )
    for r, top, bottom, p, ok, keep in tiles:
        def emit(f, v, r=r, ok=ok, keep=keep):
            if keep is not None:
                edge_ref[f, keep] = v.astype(BF16)
            act = norm_act(v, cols_ref[1])
            if ok is not None:
                act = jnp.where(ok, act, 0.0)
            act_ref[f, r] = act.astype(BF16)

        up_tile(top, bottom, p, wup_ref, cols_ref, emit)
    for f in range(2):
        hidden_frame(lambda i, r: act_ref[i, r], f, w1_ref, cols_ref, hid_ref, has_top, has_bottom)


def raw_rows(inner_ref, edge_ref, first):
    def load(f, r):
        if r in (0, 7):
            return edge_ref[first + f, r // 7]
        return inner_ref[first + f, r - 1]

    return load


def second_kernel(flags, old_ref, wup_ref, weave_ref, w1_ref, w2_ref, cols_ref, act_ref, inner_ref, edge_ref, new_ref,
                  hid_ref, out_ref, past_act_ref, rows_ref, both_ref, mix_ref, res_ref, sems):
    has_top, has_bottom, has_old = flags[0] > 0, flags[1] > 0, flags[2] > 0
    for k in range(4):
        both = old_ref[:, k]
        rows_ref[:, 2 * k] = both[..., :192]
        rows_ref[:, 2 * k + 1] = both[..., 192:]
    for i in range(0, 6, 2):
        for p in range(2):
            def emit(n, v, i=i, p=p):
                at = i + n % 2
                ok = has_old
                if at == 0:
                    ok = jnp.logical_and(ok, has_top)
                if at == 5:
                    ok = jnp.logical_and(ok, has_bottom)
                past_act_ref[n // 2, 2 * at + p] = jnp.where(ok, norm_act(v, cols_ref[1]), 0.0).astype(BF16)

            up_tile(rows_ref[:, i + p:i + p + 2], rows_ref[:, i + p + 1:i + p + 3], p, wup_ref, cols_ref, emit)

    def act(f, r):
        return past_act_ref[f, r] if f < 2 else act_ref[f - 2, r]

    def hid(f, r):
        return hid_ref[f, r] if f < 2 else new_ref[f - 2, r]

    for f in range(2):
        hidden_frame(act, f, w1_ref, cols_ref, hid_ref, has_top, has_bottom)
    decoded_frames(hid, w2_ref, weave_ref, cols_ref, raw_rows(inner_ref, edge_ref, 2), both_ref, mix_ref, res_ref, out_ref, 2,
                   sems)


def third_kernel(w2_ref, weave_ref, cols_ref, inner_ref, edge_ref, past_ref, hid_ref, _, out_ref, both_ref, mix_ref, res_ref, sems):
    def hid(f, r):
        return past_ref[f, r] if f < 2 else hid_ref[f - 2, r]

    decoded_frames(hid, w2_ref, weave_ref, cols_ref, raw_rows(inner_ref, edge_ref, 0), both_ref, mix_ref, res_ref, out_ref, 0,
                   sems)


def shape(*dims, dtype=BF16):
    return jax.ShapeDtypeStruct(dims, dtype)


def call(kernel, name, flops, in_specs, out_shape, out_specs, scratch=(), **kw):
    return pl.pallas_call(
        kernel,
        out_shape=out_shape,
        in_specs=in_specs,
        out_specs=out_specs,
        scratch_shapes=list(scratch),
        compiler_params=pltpu.CompilerParams(vmem_limit_bytes=48 << 20),
        cost_estimate=pl.CostEstimate(flops=flops, transcendentals=0, bytes_accessed=4 << 20),
        name=name,
        **kw,
    )


def shards(coarse, up_weight, up_bias, gain_one, conv_one, bias_one, gain_two, conv_two, bias_two):
    tiles, slabs = lax.axis_size("tile"), lax.axis_size("slab")
    later = [(i, i + 1) for i in range(slabs - 1)]
    x = coarse.transpose(1, 2, 3, 0)
    low, high = (jnp.concatenate([x[:, i], x[:, i + 1]], axis=2) for i in (0, 2))
    above = lax.ppermute(high, "tile", [(i, i + 1) for i in range(tiles - 1)])
    below = lax.ppermute(low, "tile", [(i + 1, i) for i in range(tiles - 1)])
    wup, w1, w2, cols, inner_act, inner_raw = call(
        prep_kernel, "prep", 2 << 30, [VMEM, VMEM, HBM, HBM] + [VMEM] * 5,
        (shape(4, 4 * CH, 192), shape(3 * CH, 9 * CH), shape(3 * CH, 9 * CH), shape(5, CH, 128, dtype=F32),
         shape(4, 6, CH, 128), shape(4, 6, CH, 128)), (VMEM,) * 6,
        [pltpu.VMEM((3, 3, CH, 3 * CH), BF16), pltpu.VMEM((3, 3, CH, 3 * CH), BF16), pltpu.SemaphoreType.DMA((2,))],
    )(x, up_weight, conv_one, conv_two, *(v.reshape(1, CH) for v in (up_bias, gain_one, bias_one, gain_two, bias_two)))
    weave = jnp.asarray(weave_matrix(), BF16)
    place, age = lax.axis_index("tile"), lax.axis_index("slab")
    flags = jnp.stack([place, tiles - 1 - place, age]).astype(jnp.int32)
    old = lax.ppermute(jnp.stack([above[2:], low[2:], high[2:], below[2:]], axis=1), "slab", later)
    act, edge_raw, new = call(
        first_kernel, "first", 3 << 30, [SMEM] + [VMEM] * 7,
        (shape(4, 12, CH, 128), shape(4, 2, CH, 128), shape(2, 10, CH, 128)), (VMEM,) * 3,
    )(flags, x, above, below, wup, w1, cols, inner_act)
    past = lax.ppermute(new, "slab", later)
    results = [pltpu.VMEM((2, 4 * CH, 256), BF16), pltpu.VMEM((2, CH * 8, 128), F32), pltpu.VMEM((CH, 2, 8, 128), BF16), pltpu.SemaphoreType.DMA((2,))]
    hid, out = call(
        second_kernel, "second", 3 << 30, [SMEM] + [VMEM] * 10,
        (shape(2, 10, CH, 128), shape(CH, 4, 8, 128)), (VMEM, ANY),
        [pltpu.VMEM((2, 12, CH, 128), BF16), pltpu.VMEM((2, 8, 64, 192), BF16)] + results,
    )(flags, old, wup, weave, w1, w2, cols, act, inner_raw, edge_raw, new)
    return call(
        third_kernel, "third", 1 << 30, [VMEM] * 7 + [ANY],
        shape(CH, 4, 8, 128), ANY, results, input_output_aliases={7: 0},
    )(w2, weave, cols, inner_raw, edge_raw, past, hid, out)


def solution(mesh):
    return jax.shard_map(
        shards,
        mesh=mesh,
        in_specs=(P(None, "slab", "tile", None), P(), P(), P(), P(), P(), P(), P(), P()),
        out_specs=P(None, "slab", "tile", None),
        check_vma=False,
    )
```

```python
import jax
import jax.numpy as jnp
import numpy as np
from jax import lax
from jax.experimental import pallas as pl
from jax.experimental.pallas import tpu as pltpu
from jax.sharding import PartitionSpec as P

F32 = jnp.float32
BF16 = jnp.bfloat16
CH = 96
VMEM = pl.BlockSpec(memory_space=pltpu.VMEM)
SMEM = pl.BlockSpec(memory_space=pltpu.SMEM)
ANY = pl.BlockSpec(memory_space=pl.ANY)
HBM = pl.BlockSpec(memory_space=pltpu.HBM)


def silu(y):
    return y * (0.5 + 0.5 * jnp.tanh(0.5 * y))


def norm_act(v, gain):
    meansq = jnp.sum(v * v, axis=0, keepdims=True) * (1.0 / CH)
    return silu(v * lax.rsqrt(meansq + 1e-06) * gain)


def lanes_of(shape):
    return lax.broadcasted_iota(jnp.int32, shape, 1)


def weave_matrix():
    m = np.zeros((256, 256), np.float32)
    for h in range(2):
        for q in range(2):
            for j in range(64):
                m[h * 128 + q * 64 + j, h * 128 + 2 * j + q] = 1
    return m


def up_tile(top, bottom, p, wup_ref, cols_ref, emit):
    lane = lanes_of((CH, 128))
    dims = (((1,), (1,)), ((), ()))
    u = lax.dot_general(wup_ref[2 * p], top.reshape(256, 192), dims, preferred_element_type=F32)
    u = u + lax.dot_general(wup_ref[2 * p + 1], bottom.reshape(256, 192), dims, preferred_element_type=F32)
    for g in range(2):
        part = u[:, 128 * g:128 * g + 128]
        even = part[:CH] + jnp.where(lane % 64 == 0, 0.0, pltpu.roll(part[CH:2 * CH], 1, 1)) + cols_ref[0]
        odd = part[2 * CH:3 * CH] + jnp.where(lane % 64 == 63, 0.0, pltpu.roll(part[3 * CH:], 127, 1)) + cols_ref[0]
        even, odd = even.astype(BF16).astype(F32), odd.astype(BF16).astype(F32)
        emit(2 * g, jnp.where(lane < 64, even, pltpu.roll(odd, 64, 1)))
        emit(2 * g + 1, jnp.where(lane < 64, pltpu.roll(even, 64, 1), odd))


def conv_pair(src, w_ref, f, r, s):
    taps = [
        jnp.concatenate([src(f + t, r + a), src(f + t, s + a)], axis=1)
        for t in range(3) for a in range(3)
    ]
    sums = jnp.dot(w_ref[...], jnp.concatenate(taps, axis=0), preferred_element_type=F32)
    lane = lanes_of((CH, 128))
    edge = jnp.logical_or(lane == 0, lane == 127)
    rows = []
    for h in range(2):
        part = sums[:, 128 * h:128 * h + 128]
        left, right = part[:CH], part[2 * CH:]
        near = pltpu.roll(jnp.where(lane < 64, left, right), 64, 1)
        far = jnp.where(lane < 64, right, left)
        far = jnp.where(lane < 64, pltpu.roll(far, 65, 1), pltpu.roll(far, 63, 1))
        rows.append(part[CH:2 * CH] + near + jnp.where(edge, 0.0, far))
    return rows


def hidden_frame(src, f, pairs, w_ref, cols_ref, hid_ref, has_top, has_bottom):
    for pair in pairs:
        rows = conv_pair(src, w_ref, f, *pair)
        for q, row in zip(pair, rows):
            act = norm_act(row + cols_ref[2], cols_ref[3])
            if q == 0 and has_top is not None:
                act = jnp.where(has_top, act, 0.0)
            if q == 9 and has_bottom is not None:
                act = jnp.where(has_bottom, act, 0.0)
            hid_ref[f, q] = act.astype(BF16)


def decoded_frames(src, w_ref, weave_ref, cols_ref, raw, both_ref, mix_ref, res_ref, done):
    def finish(f):
        woven = jnp.dot(both_ref[f], weave_ref[...], preferred_element_type=F32)
        for r in range(8):
            at, h = CH * (r // 2), 128 * (r % 2)
            mix_ref[f, pl.ds(r, CH, stride=8), :] = woven[at:at + CH, h:h + 128]
        res_ref[:, f] = mix_ref[f].reshape(CH, 8, 128).astype(BF16)
        done(f)

    for n in range(8):
        f, pair = n // 4, n % 4
        rows = conv_pair(src, w_ref, f, 2 * pair, 2 * pair + 1)
        res = [raw(f, 2 * pair + h).astype(F32) + rows[h] + cols_ref[4] for h in range(2)]
        both_ref[f, CH * pair:CH * pair + CH] = jnp.concatenate([v.astype(BF16) for v in res], axis=1)
        if n == 5:
            finish(0)
    finish(1)


def prep_kernel(x_ref, up_ref, one_ref, two_ref, upb_ref, g1_ref, b1_ref, g2_ref, b2_ref,
                wup_ref, w1_ref, w2_ref, cols_ref, act_ref, raw_ref, hid_ref, one_buf, two_buf, sems):
    loads = [
        pltpu.make_async_copy(one_ref, one_buf, sems.at[0]),
        pltpu.make_async_copy(two_ref, two_buf, sems.at[1]),
    ]
    for load in loads:
        load.start()
    for n in range(4):
        taps = []
        for b in range(3):
            if n == 0:
                tap = up_ref[0, b].astype(F32)
            elif n == 3:
                tap = up_ref[2, b].astype(F32)
            else:
                tap = up_ref[1, b].astype(F32) + up_ref[2 if n == 1 else 0, b].astype(F32)
            taps.append(tap)
        for m, tap in enumerate((taps[1] + taps[2], taps[0], taps[0] + taps[1], taps[2])):
            wup_ref[n, CH * m:CH * m + CH, :] = tap.astype(BF16)
    for n, ref in enumerate((upb_ref, g1_ref, b1_ref, g2_ref, b2_ref)):
        cols_ref[n] = jnp.broadcast_to(ref[...], (128, CH)).T
    for k in range(3):
        for n, p in enumerate((1, 0)):
            def emit(f, v, to=2 * k + n):
                raw_ref[f, to] = v.astype(BF16)
                act_ref[f, to] = norm_act(v, cols_ref[1]).astype(BF16)

            up_tile(x_ref[:, k], x_ref[:, k + 1], p, wup_ref, cols_ref, emit)
    for load, src_ref, dst_ref in ((loads[0], one_buf, w1_ref), (loads[1], two_buf, w2_ref)):
        load.wait()
        for b in range(3):
            pieces = [src_ref[t, a][:, CH * b:CH * b + CH] for t in range(3) for a in range(3)]
            dst_ref[CH * b:CH * b + CH, :] = jnp.concatenate(pieces, axis=1)
    for f in range(2):
        hidden_frame(lambda i, r: act_ref[i, r], f, ((0, 1), (2, 3)), w1_ref, cols_ref, hid_ref, None, None)


def first_kernel(flags, x_ref, above_ref, below_ref, wup_ref, w1_ref, cols_ref, inner_ref, inner_hid_ref,
                 act_ref, edge_ref, hid_ref):
    has_top, has_bottom = flags[0] > 0, flags[1] > 0
    act_ref[:, 3:9] = inner_ref[...]
    hid_ref[:, 3:7] = inner_hid_ref[...]
    above, below = above_ref[...], below_ref[...]
    above, below = (above[..., :192], above[..., 192:]), (below[..., :192], below[..., 192:])
    tiles = (
        (0, above[0], above[1], 0, has_top, None),
        (1, above[1], x_ref[:, 0], 1, has_top, None),
        (2, above[1], x_ref[:, 0], 0, None, 0),
        (9, x_ref[:, 3], below[0], 1, None, 1),
        (10, x_ref[:, 3], below[0], 0, has_bottom, None),
        (11, below[0], below[1], 1, has_bottom, None),
    )
    for r, top, bottom, p, ok, keep in tiles:
        def emit(f, v, r=r, ok=ok, keep=keep):
            if keep is not None:
                edge_ref[f, keep] = v.astype(BF16)
            act = norm_act(v, cols_ref[1])
            if ok is not None:
                act = jnp.where(ok, act, 0.0)
            act_ref[f, r] = act.astype(BF16)

        up_tile(top, bottom, p, wup_ref, cols_ref, emit)
    for f in range(2):
        hidden_frame(lambda i, r: act_ref[i, r], f, ((0, 1), (2, 7), (8, 9)), w1_ref, cols_ref, hid_ref, has_top,
                     has_bottom)


def raw_rows(inner_ref, edge_ref, first):
    def load(f, r):
        if r in (0, 7):
            return edge_ref[first + f, r // 7]
        return inner_ref[first + f, r - 1]

    return load


def second_kernel(flags, old_ref, wup_ref, weave_ref, w1_ref, w2_ref, cols_ref, act_ref, inner_ref, edge_ref, new_ref,
                  hid_ref, res_ref, past_act_ref, rows_ref, both_ref, mix_ref):
    has_top, has_bottom, has_old = flags[0] > 0, flags[1] > 0, flags[2] > 0
    for k in range(4):
        both = old_ref[:, k]
        rows_ref[:, 2 * k] = both[..., :192]
        rows_ref[:, 2 * k + 1] = both[..., 192:]
    for i in range(0, 6, 2):
        for p in range(2):
            def emit(n, v, i=i, p=p):
                at = i + n % 2
                ok = has_old
                if at == 0:
                    ok = jnp.logical_and(ok, has_top)
                if at == 5:
                    ok = jnp.logical_and(ok, has_bottom)
                past_act_ref[n // 2, 2 * at + p] = jnp.where(ok, norm_act(v, cols_ref[1]), 0.0).astype(BF16)

            up_tile(rows_ref[:, i + p:i + p + 2], rows_ref[:, i + p + 1:i + p + 3], p, wup_ref, cols_ref, emit)

    def act(f, r):
        return past_act_ref[f, r] if f < 2 else act_ref[f - 2, r]

    def hid(f, r):
        return hid_ref[f, r] if f < 2 else new_ref[f - 2, r]

    for f in range(2):
        hidden_frame(act, f, [(r, r + 1) for r in range(0, 10, 2)], w1_ref, cols_ref, hid_ref, has_top, has_bottom)
    decoded_frames(hid, w2_ref, weave_ref, cols_ref, raw_rows(inner_ref, edge_ref, 2), both_ref, mix_ref, res_ref,
                   lambda f: None)


def third_kernel(w2_ref, weave_ref, cols_ref, inner_ref, edge_ref, past_ref, hid_ref, later_ref, out_ref,
                 both_ref, mix_ref, res_ref, sems):
    copies = [pltpu.make_async_copy(later_ref, out_ref.at[:, 2:4], sems.at[2])]
    copies[0].start()

    def hid(f, r):
        return past_ref[f, r] if f < 2 else hid_ref[f - 2, r]

    def done(f):
        copies.append(pltpu.make_async_copy(res_ref.at[:, f], out_ref.at[:, f], sems.at[f]))
        copies[-1].start()

    decoded_frames(hid, w2_ref, weave_ref, cols_ref, raw_rows(inner_ref, edge_ref, 0), both_ref, mix_ref, res_ref, done)
    for copy in copies:
        copy.wait()


def shape(*dims, dtype=BF16):
    return jax.ShapeDtypeStruct(dims, dtype)


def call(kernel, name, flops, in_specs, out_shape, out_specs, scratch=(), **kw):
    return pl.pallas_call(
        kernel,
        out_shape=out_shape,
        in_specs=in_specs,
        out_specs=out_specs,
        scratch_shapes=list(scratch),
        compiler_params=pltpu.CompilerParams(vmem_limit_bytes=48 << 20),
        cost_estimate=pl.CostEstimate(flops=flops, transcendentals=0, bytes_accessed=4 << 20),
        name=name,
        **kw,
    )


def shards(coarse, up_weight, up_bias, gain_one, conv_one, bias_one, gain_two, conv_two, bias_two):
    tiles, slabs = lax.axis_size("tile"), lax.axis_size("slab")
    onward = [(i, i + 1) for i in range(slabs - 1)]
    x = coarse.transpose(1, 2, 3, 0)
    low, high = (jnp.concatenate([x[:, i], x[:, i + 1]], axis=2) for i in (0, 2))
    above = lax.ppermute(high, "tile", [(i, i + 1) for i in range(tiles - 1)])
    below = lax.ppermute(low, "tile", [(i + 1, i) for i in range(tiles - 1)])
    wup, w1, w2, cols, inner_act, inner_raw, inner_hid = call(
        prep_kernel, "prep", 2 << 30, [VMEM, VMEM, HBM, HBM] + [VMEM] * 5,
        (shape(4, 4 * CH, 192), shape(3 * CH, 9 * CH), shape(3 * CH, 9 * CH), shape(5, CH, 128, dtype=F32),
         shape(4, 6, CH, 128), shape(4, 6, CH, 128), shape(2, 4, CH, 128)), (VMEM,) * 7,
        [pltpu.VMEM((3, 3, CH, 3 * CH), BF16), pltpu.VMEM((3, 3, CH, 3 * CH), BF16), pltpu.SemaphoreType.DMA((2,))],
    )(x, up_weight, conv_one, conv_two, *(v.reshape(1, CH) for v in (up_bias, gain_one, bias_one, gain_two, bias_two)))
    weave = jnp.asarray(weave_matrix(), BF16)
    place, age = lax.axis_index("tile"), lax.axis_index("slab")
    flags = jnp.stack([place, tiles - 1 - place, age]).astype(jnp.int32)
    old = lax.ppermute(jnp.stack([above[2:], low[2:], high[2:], below[2:]], axis=1), "slab", onward)
    act, edge_raw, new = call(
        first_kernel, "first", 3 << 30, [SMEM] + [VMEM] * 8,
        (shape(4, 12, CH, 128), shape(4, 2, CH, 128), shape(2, 10, CH, 128)), (VMEM,) * 3,
    )(flags, x, above, below, wup, w1, cols, inner_act, inner_hid)
    past = lax.ppermute(new, "slab", onward)
    work = [pltpu.VMEM((2, 4 * CH, 256), BF16), pltpu.VMEM((2, CH * 8, 128), F32)]
    hid, later = call(
        second_kernel, "second", 3 << 30, [SMEM] + [VMEM] * 10,
        (shape(2, 10, CH, 128), shape(CH, 2, 8, 128)), (VMEM, VMEM),
        [pltpu.VMEM((2, 12, CH, 128), BF16), pltpu.VMEM((2, 8, 64, 192), BF16)] + work,
    )(flags, old, wup, weave, w1, w2, cols, act, inner_raw, edge_raw, new)
    return call(
        third_kernel, "third", 1 << 30, [VMEM] * 8, shape(CH, 4, 8, 128), ANY,
        work + [pltpu.VMEM((CH, 2, 8, 128), BF16), pltpu.SemaphoreType.DMA((3,))],
    )(w2, weave, cols, inner_raw, edge_raw, past, hid, later)


def solution(mesh):
    return jax.shard_map(
        shards,
        mesh=mesh,
        in_specs=(P(None, "slab", "tile", None), P(), P(), P(), P(), P(), P(), P(), P()),
        out_specs=P(None, "slab", "tile", None),
        check_vma=False,
    )
```

```python
import jax
import jax.numpy as jnp
import numpy as np
from jax import lax
from jax.experimental import pallas as pl
from jax.experimental.pallas import tpu as pltpu
from jax.sharding import PartitionSpec as P

F32 = jnp.float32
BF16 = jnp.bfloat16
CH = 96
VMEM = pl.BlockSpec(memory_space=pltpu.VMEM)
ANY = pl.BlockSpec(memory_space=pl.ANY)
HBM = pl.BlockSpec(memory_space=pltpu.HBM)


def silu(y):
    return y * (0.5 + 0.5 * jnp.tanh(0.5 * y))


def norm_act(v, gain):
    meansq = jnp.sum(v * v, axis=0, keepdims=True) * (1.0 / CH)
    return silu(v * lax.rsqrt(meansq + 1e-06) * gain)


def lanes_of(shape):
    return lax.broadcasted_iota(jnp.int32, shape, 1)


def weave_matrix():
    m = np.zeros((256, 256), np.float32)
    for h in range(2):
        for q in range(2):
            for j in range(64):
                m[h * 128 + q * 64 + j, h * 128 + 2 * j + q] = 1
    return m


def up_tile(top, bottom, p, wup_ref, cols_ref, emit):
    lane = lanes_of((16, 128))
    dims = (((1,), (1,)), ((), ()))
    u = lax.dot_general(wup_ref[2 * p], top.reshape(256, 192), dims, preferred_element_type=F32)
    u = u + lax.dot_general(wup_ref[2 * p + 1], bottom.reshape(256, 192), dims, preferred_element_type=F32)
    for g in range(2):
        first, second = [], []
        for k in range(0, CH, 16):
            a, b, c, d = (u[4 * k + m:4 * k + m + 16, 128 * g:128 * g + 128] for m in (0, 16, 32, 48))
            even = a + jnp.where(lane % 64 == 0, 0.0, pltpu.roll(b, 1, 1)) + cols_ref[0, k:k + 16]
            odd = c + jnp.where(lane % 64 == 63, 0.0, pltpu.roll(d, 127, 1)) + cols_ref[0, k:k + 16]
            even, odd = even.astype(BF16).astype(F32), odd.astype(BF16).astype(F32)
            first.append(jnp.where(lane < 64, even, pltpu.roll(odd, 64, 1)))
            second.append(jnp.where(lane < 64, pltpu.roll(even, 64, 1), odd))
        emit(2 * g, jnp.concatenate(first, axis=0))
        emit(2 * g + 1, jnp.concatenate(second, axis=0))


def conv_pair(src, w_ref, f, r, s):
    taps = [
        jnp.concatenate([src(f + t, r + a), src(f + t, s + a)], axis=1)
        for t in range(3) for a in range(3)
    ]
    sums = jnp.dot(w_ref[...], jnp.concatenate(taps, axis=0), preferred_element_type=F32)
    lane = lanes_of((16, 128))
    edge = jnp.logical_or(lane == 0, lane == 127)
    rows = []
    for h in range(2):
        blocks = []
        for k in range(0, 3 * CH, 48):
            left, middle, right = (sums[k + b:k + b + 16, 128 * h:128 * h + 128] for b in (0, 16, 32))
            near = pltpu.roll(jnp.where(lane < 64, left, right), 64, 1)
            far = jnp.where(lane < 64, right, left)
            far = jnp.where(lane < 64, pltpu.roll(far, 65, 1), pltpu.roll(far, 63, 1))
            blocks.append(middle + near + jnp.where(edge, 0.0, far))
        rows.append(jnp.concatenate(blocks, axis=0))
    return rows


def hidden_frame(src, f, pairs, w_ref, cols_ref, hid_ref, has_top, has_bottom):
    for pair in pairs:
        rows = conv_pair(src, w_ref, f, *pair)
        for q, row in zip(pair, rows):
            act = norm_act(row + cols_ref[2], cols_ref[3])
            if q == 0 and has_top is not None:
                act = jnp.where(has_top, act, 0.0)
            if q == 9 and has_bottom is not None:
                act = jnp.where(has_bottom, act, 0.0)
            hid_ref[f, q] = act.astype(BF16)


def decoded_frames(src, w_ref, weave_ref, cols_ref, raw, both_ref, mix_ref, res_ref, done):
    def finish(f):
        woven = jnp.dot(both_ref[f], weave_ref[...], preferred_element_type=F32)
        for r in range(8):
            at, h = CH * (r // 2), 128 * (r % 2)
            mix_ref[f, pl.ds(r, CH, stride=8), :] = woven[at:at + CH, h:h + 128]
        res_ref[:, f] = mix_ref[f].reshape(CH, 8, 128).astype(BF16)
        done(f)

    for n in range(8):
        f, pair = n // 4, n % 4
        rows = conv_pair(src, w_ref, f, 2 * pair, 2 * pair + 1)
        res = [raw(f, 2 * pair + h).astype(F32) + rows[h] + cols_ref[4] for h in range(2)]
        both_ref[f, CH * pair:CH * pair + CH] = jnp.concatenate([v.astype(BF16) for v in res], axis=1)
        if n == 5:
            finish(0)
    finish(1)


def prep_kernel(x_ref, up_ref, one_ref, two_ref, upb_ref, g1_ref, b1_ref, g2_ref, b2_ref,
                wup_ref, w1_ref, w2_ref, cols_ref, act_ref, raw_ref, hid_ref, one_buf, two_buf, sems):
    loads = [
        pltpu.make_async_copy(one_ref, one_buf, sems.at[0]),
        pltpu.make_async_copy(two_ref, two_buf, sems.at[1]),
    ]
    for load in loads:
        load.start()
    for n in range(4):
        taps = []
        for b in range(3):
            if n == 0:
                tap = up_ref[0, b].astype(F32)
            elif n == 3:
                tap = up_ref[2, b].astype(F32)
            else:
                tap = up_ref[1, b].astype(F32) + up_ref[2 if n == 1 else 0, b].astype(F32)
            taps.append(tap)
        for m, tap in enumerate((taps[1] + taps[2], taps[0], taps[0] + taps[1], taps[2])):
            for k in range(0, CH, 16):
                wup_ref[n, 4 * k + 16 * m:4 * k + 16 * m + 16, :] = tap[k:k + 16].astype(BF16)
    for n, ref in enumerate((upb_ref, g1_ref, b1_ref, g2_ref, b2_ref)):
        cols_ref[n] = jnp.broadcast_to(ref[...], (128, CH)).T
    for k in range(3):
        for n, p in enumerate((1, 0)):
            def emit(f, v, to=2 * k + n):
                raw_ref[f, to] = v.astype(BF16)
                act_ref[f, to] = norm_act(v, cols_ref[1]).astype(BF16)

            up_tile(x_ref[:, k], x_ref[:, k + 1], p, wup_ref, cols_ref, emit)
    for load, src_ref, dst_ref in ((loads[0], one_buf, w1_ref), (loads[1], two_buf, w2_ref)):
        load.wait()
        for b in range(3):
            pieces = [src_ref[t, a][:, CH * b:CH * b + CH] for t in range(3) for a in range(3)]
            rows = jnp.concatenate(pieces, axis=1)
            for k in range(0, CH, 16):
                dst_ref[3 * k + 16 * b:3 * k + 16 * b + 16, :] = rows[k:k + 16]
    for f in range(2):
        hidden_frame(lambda i, r: act_ref[i, r], f, ((0, 1), (2, 3)), w1_ref, cols_ref, hid_ref, None, None)


def surroundings():
    place = lax.axis_index("tile")
    return place > 0, place < lax.axis_size("tile") - 1, lax.axis_index("slab") > 0


def first_kernel(x_ref, above_ref, below_ref, wup_ref, w1_ref, cols_ref, inner_ref, inner_hid_ref,
                 act_ref, edge_ref, hid_ref):
    has_top, has_bottom, _ = surroundings()
    act_ref[:, 3:9] = inner_ref[...]
    hid_ref[:, 3:7] = inner_hid_ref[...]
    above, below = above_ref[...], below_ref[...]
    above, below = (above[..., :192], above[..., 192:]), (below[..., :192], below[..., 192:])
    tiles = (
        (0, above[0], above[1], 0, has_top, None),
        (1, above[1], x_ref[:, 0], 1, has_top, None),
        (2, above[1], x_ref[:, 0], 0, None, 0),
        (9, x_ref[:, 3], below[0], 1, None, 1),
        (10, x_ref[:, 3], below[0], 0, has_bottom, None),
        (11, below[0], below[1], 1, has_bottom, None),
    )
    for r, top, bottom, p, ok, keep in tiles:
        def emit(f, v, r=r, ok=ok, keep=keep):
            if keep is not None:
                edge_ref[f, keep] = v.astype(BF16)
            act = norm_act(v, cols_ref[1])
            if ok is not None:
                act = jnp.where(ok, act, 0.0)
            act_ref[f, r] = act.astype(BF16)

        up_tile(top, bottom, p, wup_ref, cols_ref, emit)
    for f in range(2):
        hidden_frame(lambda i, r: act_ref[i, r], f, ((0, 1), (2, 7), (8, 9)), w1_ref, cols_ref, hid_ref, has_top,
                     has_bottom)


def raw_rows(inner_ref, edge_ref, first):
    def load(f, r):
        if r in (0, 7):
            return edge_ref[first + f, r // 7]
        return inner_ref[first + f, r - 1]

    return load


def second_kernel(old_ref, wup_ref, weave_ref, w1_ref, w2_ref, cols_ref, act_ref, inner_ref, edge_ref, new_ref,
                  hid_ref, res_ref, past_act_ref, rows_ref, both_ref, mix_ref):
    has_top, has_bottom, has_old = surroundings()
    for k in range(4):
        both = old_ref[:, k]
        rows_ref[:, 2 * k] = both[..., :192]
        rows_ref[:, 2 * k + 1] = both[..., 192:]
    for i in range(0, 6, 2):
        for p in range(2):
            def emit(n, v, i=i, p=p):
                at = i + n % 2
                ok = has_old
                if at == 0:
                    ok = jnp.logical_and(ok, has_top)
                if at == 5:
                    ok = jnp.logical_and(ok, has_bottom)
                past_act_ref[n // 2, 2 * at + p] = jnp.where(ok, norm_act(v, cols_ref[1]), 0.0).astype(BF16)

            up_tile(rows_ref[:, i + p:i + p + 2], rows_ref[:, i + p + 1:i + p + 3], p, wup_ref, cols_ref, emit)

    def act(f, r):
        return past_act_ref[f, r] if f < 2 else act_ref[f - 2, r]

    def hid(f, r):
        return hid_ref[f, r] if f < 2 else new_ref[f - 2, r]

    for f in range(2):
        hidden_frame(act, f, [(r, r + 1) for r in range(0, 10, 2)], w1_ref, cols_ref, hid_ref, has_top, has_bottom)
    decoded_frames(hid, w2_ref, weave_ref, cols_ref, raw_rows(inner_ref, edge_ref, 2), both_ref, mix_ref, res_ref,
                   lambda f: None)


def third_kernel(w2_ref, weave_ref, cols_ref, inner_ref, edge_ref, past_ref, hid_ref, later_ref, out_ref,
                 both_ref, mix_ref, res_ref, sems):
    copies = [pltpu.make_async_copy(later_ref, out_ref.at[:, 2:4], sems.at[2])]
    copies[0].start()

    def hid(f, r):
        return past_ref[f, r] if f < 2 else hid_ref[f - 2, r]

    def done(f):
        copies.append(pltpu.make_async_copy(res_ref.at[:, f], out_ref.at[:, f], sems.at[f]))
        copies[-1].start()

    decoded_frames(hid, w2_ref, weave_ref, cols_ref, raw_rows(inner_ref, edge_ref, 0), both_ref, mix_ref, res_ref, done)
    for copy in copies:
        copy.wait()


def shape(*dims, dtype=BF16):
    return jax.ShapeDtypeStruct(dims, dtype)


def call(kernel, name, flops, in_specs, out_shape, out_specs, scratch=(), **kw):
    return pl.pallas_call(
        kernel,
        out_shape=out_shape,
        in_specs=in_specs,
        out_specs=out_specs,
        scratch_shapes=list(scratch),
        compiler_params=pltpu.CompilerParams(vmem_limit_bytes=48 << 20),
        cost_estimate=pl.CostEstimate(flops=flops, transcendentals=0, bytes_accessed=4 << 20),
        name=name,
        **kw,
    )


def shards(coarse, up_weight, up_bias, gain_one, conv_one, bias_one, gain_two, conv_two, bias_two):
    tiles, slabs = lax.axis_size("tile"), lax.axis_size("slab")
    onward = [(i, i + 1) for i in range(slabs - 1)]
    x = coarse.transpose(1, 2, 3, 0)
    low, high = (jnp.concatenate([x[:, i], x[:, i + 1]], axis=2) for i in (0, 2))
    above = lax.ppermute(high, "tile", [(i, i + 1) for i in range(tiles - 1)])
    below = lax.ppermute(low, "tile", [(i + 1, i) for i in range(tiles - 1)])
    wup, w1, w2, cols, inner_act, inner_raw, inner_hid = call(
        prep_kernel, "prep", 2 << 30, [VMEM, VMEM, HBM, HBM] + [VMEM] * 5,
        (shape(4, 4 * CH, 192), shape(3 * CH, 9 * CH), shape(3 * CH, 9 * CH), shape(5, CH, 128, dtype=F32),
         shape(4, 6, CH, 128), shape(4, 6, CH, 128), shape(2, 4, CH, 128)), (VMEM,) * 7,
        [pltpu.VMEM((3, 3, CH, 3 * CH), BF16), pltpu.VMEM((3, 3, CH, 3 * CH), BF16), pltpu.SemaphoreType.DMA((2,))],
    )(x, up_weight, conv_one, conv_two, *(v.reshape(1, CH) for v in (up_bias, gain_one, bias_one, gain_two, bias_two)))
    weave = jnp.asarray(weave_matrix(), BF16)
    old = lax.ppermute(jnp.stack([above[2:], low[2:], high[2:], below[2:]], axis=1), "slab", onward)
    act, edge_raw, new = call(
        first_kernel, "first", 3 << 30, [VMEM] * 8,
        (shape(4, 12, CH, 128), shape(4, 2, CH, 128), shape(2, 10, CH, 128)), (VMEM,) * 3,
    )(x, above, below, wup, w1, cols, inner_act, inner_hid)
    past = lax.ppermute(new, "slab", onward)
    work = [pltpu.VMEM((2, 4 * CH, 256), BF16), pltpu.VMEM((2, CH * 8, 128), F32)]
    hid, later = call(
        second_kernel, "second", 3 << 30, [VMEM] * 10,
        (shape(2, 10, CH, 128), shape(CH, 2, 8, 128)), (VMEM, VMEM),
        [pltpu.VMEM((2, 12, CH, 128), BF16), pltpu.VMEM((2, 8, 64, 192), BF16)] + work,
    )(old, wup, weave, w1, w2, cols, act, inner_raw, edge_raw, new)
    return call(
        third_kernel, "third", 1 << 30, [VMEM] * 8, shape(CH, 4, 8, 128), ANY,
        work + [pltpu.VMEM((CH, 2, 8, 128), BF16), pltpu.SemaphoreType.DMA((3,))],
    )(w2, weave, cols, inner_raw, edge_raw, past, hid, later)


def solution(mesh):
    return jax.shard_map(
        shards,
        mesh=mesh,
        in_specs=(P(None, "slab", "tile", None), P(), P(), P(), P(), P(), P(), P(), P()),
        out_specs=P(None, "slab", "tile", None),
        check_vma=False,
    )
```
